8 devices in a mesh: dp: 1 (over z), tp: 8 (over y, x, core).
Axes of the slice: x: 2, y: 2, z: 1, core: 2. Of those that a mesh axis runs over, the one named last changes fastest.
Arguments:
- residual: float32 [256, 4096], P('dp')
- norm_w: bfloat16 [2, 4096], replicated
- w_in: bfloat16 [2, 4096, 2, 8192], P(None, None, None, 'tp')
- conv_w: bfloat16 [2, 4, 8192], P(None, None, 'tp')
- conv_b: bfloat16 [2, 8192], P(None, 'tp')
- w_x: bfloat16 [2, 8192, 288], P(None, 'tp')
- w_dt: bfloat16 [2, 256, 8192], P(None, None, 'tp')
- b_dt: float32 [2, 8192], P(None, 'tp')
- a_log: float32 [2, 16, 8192], P(None, None, 'tp')
- d_skip: float32 [2, 8192], P(None, 'tp')
- w_out: bfloat16 [2, 8192, 4096], P(None, 'tp')
- conv_state: bfloat16 [2, 256, 3, 8192], P(None, 'dp', None, 'tp')
- ssm_state: float32 [2, 256, 16, 8192], P(None, 'dp', None, 'tp')
Outputs:
- output 1: float32 [256, 4096], P('dp')
- output 2: bfloat16 [2, 256, 3, 8192], P(None, 'dp', None, 'tp')
- output 3: float32 [2, 256, 16, 8192], P(None, 'dp', None, 'tp')
All inputs are finite; a program needn't handle non-finite values.
Results may differ from the reference program's by a relative error of at most 0.0192232.
Values are sent between devices in bfloat16 or wider.
A program may use at most 1 GiB of HBM per device.

```python
import math
import jax
import jax.numpy as jnp
from jax import lax

D = 4096
INNER = 8192
STATE = 16
RANK = 256
CONV = 4
LAYERS = 2
BATCH = 256


def setup_inputs(seed: int = 0, part: int = 0) -> dict:
    root_key = jax.random.key(seed)
    shared = jax.random.split(root_key, 10)
    part_keys = jax.random.split(jax.random.fold_in(root_key, part), 3)
    proj_width = RANK + 2 * STATE
    residual = jax.random.normal(part_keys[0], (BATCH, D), jnp.float32)
    norm_w = jax.random.uniform(shared[0], (LAYERS, D), jnp.float32, 0.5, 1.5).astype(jnp.bfloat16)
    w_in = (jax.random.normal(shared[1], (LAYERS, D, 2, INNER), jnp.float32) * D ** -0.5).astype(jnp.bfloat16)
    conv_w = (0.5 * jax.random.normal(shared[2], (LAYERS, CONV, INNER), jnp.float32)).astype(jnp.bfloat16)
    conv_b = (0.3 * jax.random.normal(shared[3], (LAYERS, INNER), jnp.float32)).astype(jnp.bfloat16)
    w_x = (jax.random.normal(shared[4], (LAYERS, INNER, proj_width), jnp.float32) * INNER ** -0.5).astype(jnp.bfloat16)
    w_dt = (jax.random.normal(shared[5], (LAYERS, RANK, INNER), jnp.float32) * (0.25 * RANK ** -0.5)).astype(jnp.bfloat16)
    dt_init = jnp.exp(jax.random.uniform(shared[6], (LAYERS, INNER), jnp.float32, math.log(0.05), math.log(0.25)))
    b_dt = dt_init + jnp.log(-jnp.expm1(-dt_init))
    a_log = jax.random.uniform(shared[7], (LAYERS, STATE, INNER), jnp.float32, -0.7, 0.7)
    d_skip = jax.random.uniform(shared[8], (LAYERS, INNER), jnp.float32, 0.5, 1.5)
    w_out = (jax.random.normal(shared[9], (LAYERS, INNER, D), jnp.float32) * INNER ** -0.5).astype(jnp.bfloat16)
    conv_state = jax.random.normal(part_keys[1], (LAYERS, BATCH, CONV - 1, INNER), jnp.float32).astype(jnp.bfloat16)
    ssm_state = 0.5 * jax.random.normal(part_keys[2], (LAYERS, BATCH, STATE, INNER), jnp.float32)
    return {'residual': residual, 'norm_w': norm_w, 'w_in': w_in, 'conv_w': conv_w, 'conv_b': conv_b, 'w_x': w_x, 'w_dt': w_dt, 'b_dt': b_dt, 'a_log': a_log, 'd_skip': d_skip, 'w_out': w_out, 'conv_state': conv_state, 'ssm_state': ssm_state}


def rms_norm(vector, epsilon):
    return vector * lax.rsqrt(jnp.mean(vector * vector, axis=-1, keepdims=True) + epsilon)


def mamba_layer(residual, params):
    norm_w, w_in, conv_w, conv_b, w_x, w_dt, b_dt, a_log, d_skip, w_out, conv_state, ssm_state = params
    hidden = (rms_norm(residual, 1e-5) * norm_w.astype(jnp.float32)).astype(jnp.bfloat16)
    x_part = jnp.dot(hidden, w_in[:, 0, :], preferred_element_type=jnp.float32).astype(jnp.bfloat16)
    z_part = jnp.dot(hidden, w_in[:, 1, :], preferred_element_type=jnp.float32).astype(jnp.bfloat16)
    window = jnp.concatenate([conv_state, x_part[:, None, :]], axis=1)
    conv_pre = jnp.sum(window.astype(jnp.float32) * conv_w.astype(jnp.float32)[None], axis=1) + conv_b.astype(jnp.float32)
    x_conv = jax.nn.silu(conv_pre).astype(jnp.bfloat16)
    proj_sum = jnp.dot(x_conv, w_x, preferred_element_type=jnp.float32)
    dt_low = rms_norm(proj_sum[:, :RANK], 1e-6).astype(jnp.bfloat16)
    b_vec = rms_norm(proj_sum[:, RANK:RANK + STATE], 1e-6)
    c_vec = rms_norm(proj_sum[:, RANK + STATE:], 1e-6)
    dt_val = jax.nn.softplus(jnp.dot(dt_low, w_dt, preferred_element_type=jnp.float32) + b_dt)
    x_float = x_conv.astype(jnp.float32)
    decay_fac = jnp.exp(dt_val[:, None, :] * -jnp.exp(a_log)[None])
    new_ssm = decay_fac * ssm_state + (dt_val * x_float)[:, None, :] * b_vec[:, :, None]
    y_val = jnp.sum(new_ssm * c_vec[:, :, None], axis=1) + d_skip * x_float
    gated_y = (y_val * jax.nn.silu(z_part.astype(jnp.float32))).astype(jnp.bfloat16)
    out_sum = jnp.dot(gated_y, w_out, preferred_element_type=jnp.float32)
    return residual + out_sum, (window[:, 1:, :], new_ssm)


def reference(residual, norm_w, w_in, conv_w, conv_b, w_x, w_dt, b_dt, a_log, d_skip, w_out, conv_state, ssm_state):
    resid_out, cache_new = lax.scan(mamba_layer, residual, (norm_w, w_in, conv_w, conv_b, w_x, w_dt, b_dt, a_log, d_skip, w_out, conv_state, ssm_state))
    return resid_out, cache_new[0], cache_new[1]
```

```python
import functools

import jax
import jax.numpy as jnp
from jax import lax
from jax.experimental import pallas as pl
from jax.experimental.pallas import tpu as pltpu
from jax.sharding import PartitionSpec as P

F32 = jnp.float32
BF16 = jnp.bfloat16
MESH = pl.DeviceIdType.MESH
VMEM = pl.BlockSpec(memory_space=pltpu.VMEM)
ANY = pl.BlockSpec(memory_space=pl.ANY)
DMA = pltpu.SemaphoreType.DMA

TOK = 256
DIM = 4096
CH = 1024
PW = 288
NST = 16
RANK = 256
NCH = 4
CW = DIM // NCH
NW = 8
KD = 256


def rows(start, size):
    return pl.ds(pl.multiple_of(start, size), size)


def place():
    me = lax.axis_index("tp")
    core = lax.rem(me, 2)
    xb = lax.rem(lax.div(me, 2), 2)
    yb = lax.div(me, 4)
    partner = me + 1 - 2 * core
    xn = me + 2 - 4 * xb
    yn = me + 4 - 8 * yb
    first = xn * (1 - core) + yn * core
    second = yn * (1 - core) + xn * core
    fb = xb * (1 - core) + yb * core
    sb = yb * (1 - core) + xb * core
    return core, fb, sb, partner, first, second


def enter(peers):
    barrier = pltpu.get_barrier_semaphore()
    for peer in peers:
        pl.semaphore_signal(barrier, inc=1, device_id={"tp": peer}, device_id_type=MESH)
    return lambda: pl.semaphore_wait(barrier, len(peers))


def remote(src, dst, sems, idx, to):
    return pltpu.make_async_remote_copy(
        src_ref=src, dst_ref=dst, send_sem=sems.at[0, idx], recv_sem=sems.at[1, idx],
        device_id={"tp": to}, device_id_type=MESH)


def spread(parity):
    src = lax.broadcasted_iota(jnp.int32, (128, 256), 0)
    dst = lax.broadcasted_iota(jnp.int32, (128, 256), 1)
    return jnp.where(dst == 2 * src + parity, 1.0, 0.0).astype(BF16)


def proj_steps(lo, hi, parity, acc, h, w):
    sel = spread(parity)

    def step(i, carry):
        cols = rows(i * KD, KD)
        hc = h[:, cols]
        lhs = jnp.concatenate(
            [jnp.dot(hc[:, j * 128:(j + 1) * 128], sel, preferred_element_type=F32).astype(BF16)
             for j in range(KD // 128)], axis=1)
        wc = w[cols].reshape(2 * KD, CH)
        acc[...] += jnp.dot(lhs, wc, preferred_element_type=F32)
        return carry

    lax.fori_loop(lo, hi, step, 0)


def w_in_copies(layer, w_in, w, sem):
    size = DIM // NW
    return [pltpu.make_async_copy(w_in.at[layer, pl.ds(i * size, size)], w.at[pl.ds(i * size, size)], sem.at[i])
            for i in range(NW)]


def conv_stage(acc, cs, conv_w, conv_b, x, xc):
    def block(i, carry):
        r = rows(i * 32, 32)
        xv = acc[r, :].astype(BF16)
        x[r, :] = xv
        pre = cs[0, r, :].astype(F32) * conv_w[0:1, :]
        pre += cs[1, r, :].astype(F32) * conv_w[1:2, :]
        pre += cs[2, r, :].astype(F32) * conv_w[2:3, :]
        pre += xv.astype(F32) * conv_w[3:4, :]
        pre += conv_b[...]
        xc[r, :] = (pre * jax.nn.sigmoid(pre)).astype(BF16)
        return carry

    lax.fori_loop(0, TOK // 32, block, 0)


def p_stage(where, z_part, xc, wx, p, ptx, prx, psem):
    core, _, _, partner, first, second = where

    def half(index):
        return lax.dot_general(wx[...], xc[rows(index * 128, 128), :], (((1,), (1,)), ((), ())),
                               preferred_element_type=F32)

    ptx[0] = half(1 - core).astype(BF16)
    hop = remote(ptx.at[0], prx.at[0], psem, 0, partner)
    hop.start()
    p[core] = half(core)
    z_part(0)
    hop.wait()
    for k, to in ((1, first), (2, second), (3, partner)):
        p[core] += prx[k - 1].astype(F32)
        ptx[k] = p[core].astype(BF16)
        hop = remote(ptx.at[k], prx.at[k], psem, k, to)
        hop.start()
        z_part(k)
        hop.wait()
    p[1 - core] = prx[3].astype(F32)


def in_tail(where, acc, h, w, cs, conv_w, conv_b, wx, x, xc, z, p, ptx, prx, psem):
    conv_stage(acc, cs, conv_w, conv_b, x, xc)
    acc[...] = jnp.zeros_like(acc)
    n = DIM // KD
    cuts = (0, n // 8, n // 2, n - n // 8, n)

    def z_part(k):
        proj_steps(cuts[k], cuts[k + 1], 1, acc, h, w)

    p_stage(where, z_part, xc, wx, p, ptx, prx, psem)

    def block(i, carry):
        r = rows(i * 32, 32)
        z[r, :] = acc[r, :].astype(BF16)
        return carry

    lax.fori_loop(0, TOK // 32, block, 0)


def first_kernel(resid, norm_w, w_in, conv_w, conv_b, wx_hbm, cs_hbm, x, xc, z, p,
                 h, w, acc, rbuf, wx, cs, ptx, prx, wsem, lsem, psem):
    where = place()
    core, fb, sb, partner, first, second = where
    await_peers = enter((partner, first, second))
    nr = 8
    rcopies = [pltpu.make_async_copy(resid.at[pl.ds(i * 32, 32)], rbuf.at[pl.ds(i * 32, 32)], lsem.at[2 + i])
               for i in range(nr)]
    for c in rcopies:
        c.start()
    wcopies = w_in_copies(0, w_in, w, wsem)
    for c in wcopies:
        c.start()
    small = [pltpu.make_async_copy(wx_hbm.at[0], wx, lsem.at[0]), pltpu.make_async_copy(cs_hbm.at[0], cs, lsem.at[1])]
    for c in small:
        c.start()
    acc[...] = jnp.zeros_like(acc)

    for c in rcopies:
        c.wait()

    def norm_block(i, carry):
        r = rows(i * 16, 16)
        v = rbuf[r, :]
        scale = lax.rsqrt(jnp.mean(v * v, axis=-1, keepdims=True) + 1e-5)
        h[r, :] = (v * scale * norm_w[...]).astype(BF16)
        return carry

    lax.fori_loop(0, TOK // 16, norm_block, 0)
    per = DIM // NW // KD
    for i in range(NW):
        wcopies[i].wait()
        proj_steps(i * per, (i + 1) * per, 0, acc, h, w)
    for c in small:
        c.wait()
    await_peers()
    in_tail(where, acc, h, w, cs, conv_w, conv_b, wx, x, xc, z, p, ptx, prx, psem)


def reduce_scatter(where, await_peers, yg, wout, wcopies, own, tx0, rx0, tx1, rx1, tx2, rx2, rsem):
    core, fb, sb, partner, first, second = where
    col = [pl.ds(c * CW, CW) for c in range(NCH)]
    hop0 = [remote(tx0.at[:, col[c]], rx0.at[:, col[c]], rsem, c, partner) for c in range(NCH)]
    hop1 = [remote(tx1.at[:, col[c]], rx1.at[:, col[c]], rsem, NCH + c, first) for c in range(NCH)]
    hop2 = [remote(tx2.at[:, col[c]], rx2.at[:, col[c]], rsem, 2 * NCH + c, second) for c in range(NCH)]

    def product(c):
        wcopies[c].wait()
        wc = wout[:, col[c]]
        tx0[:, col[c]] = jnp.dot(yg[rows((1 - core) * 128, 128), :], wc, preferred_element_type=F32).astype(BF16)
        if c == 0:
            await_peers()
        hop0[c].start()
        own[:, col[c]] = jnp.dot(yg[rows(core * 128, 128), :], wc, preferred_element_type=F32)

    def stage1(c):
        hop0[c].wait()
        give, keep = rows((1 - fb) * 64, 64), rows(fb * 64, 64)
        tx1[:, col[c]] = (own[give, col[c]] + rx0[give, col[c]].astype(F32)).astype(BF16)
        hop1[c].start()
        own[keep, col[c]] += rx0[keep, col[c]].astype(F32)

    def stage2(c):
        hop1[c].wait()
        give, keep = (1 - sb) * 32, sb * 32
        tx2[:, col[c]] = (own[rows(fb * 64 + give, 32), col[c]] + rx1[rows(give, 32), col[c]].astype(F32)).astype(BF16)
        hop2[c].start()
        own[rows(fb * 64 + keep, 32), col[c]] += rx1[rows(keep, 32), col[c]].astype(F32)

    product(0)
    product(1)
    stage1(0)
    product(2)
    stage1(1)
    product(3)
    stage1(2)
    stage1(3)
    for c in range(NCH):
        stage2(c)
    mine = rows(fb * 64 + sb * 32, 32)
    for c in range(NCH):
        hop2[c].wait()
        own[mine, col[c]] += rx2[:, col[c]].astype(F32)
    return mine


def all_gather(where, h, gsem, consume):
    core, fb, sb, partner, first, second = where
    col = [pl.ds(c * CW, CW) for c in range(NCH)]
    base = core * 128

    def hops(k, start, size, to):
        part = [h.at[rows(start, size), col[c]] for c in range(NCH)]
        return [remote(part[c], part[c], gsem, k * NCH + c, to) for c in range(NCH)]

    hop0 = hops(0, base + fb * 64 + sb * 32, 32, second)
    hop1 = hops(1, base + fb * 64, 64, first)
    hop2 = hops(2, base, 128, partner)
    for c in range(NCH):
        hop0[c].start()
    for c in range(NCH):
        hop0[c].wait()
        hop1[c].start()
    for c in range(NCH):
        hop1[c].wait()
        hop2[c].start()
    for c in range(NCH):
        hop2[c].wait()
        consume(c)


def w_out_copies(layer, w_out, wout, sem):
    return [pltpu.make_async_copy(w_out.at[layer, :, pl.ds(c * CW, CW)], wout.at[:, pl.ds(c * CW, CW)], sem.at[c])
            for c in range(NCH)]


def middle_kernel(yg, w_out, resid, norm_w, w_in, conv_w, conv_b, wx_hbm, cs_hbm, x, xc, z, p, oshard,
                  wout, own, tx0, rx0, tx1, rx1, tx2, rx2, rmine,
                  h, w, acc, wx, cs, ptx, prx, osem, wsem, lsem, rsem, gsem, psem):
    where = place()
    core, fb, sb, partner, first, second = where
    await_peers = enter((partner, first, second))
    ocopies = w_out_copies(0, w_out, wout, osem)
    for c in ocopies:
        c.start()
    row0 = core * 128 + fb * 64 + sb * 32
    small = [pltpu.make_async_copy(wx_hbm.at[1], wx, lsem.at[0]), pltpu.make_async_copy(cs_hbm.at[1], cs, lsem.at[1]),
             pltpu.make_async_copy(resid.at[rows(row0, 32)], rmine, lsem.at[2])]
    for c in small:
        c.start()
    wcopies = w_in_copies(1, w_in, w, wsem)
    for c in wcopies:
        c.start()
    acc[...] = jnp.zeros_like(acc)
    mine = reduce_scatter(where, await_peers, yg, wout, ocopies, own, tx0, rx0, tx1, rx1, tx2, rx2, rsem)
    small[2].wait()
    for b in range(2):
        sub = pl.ds(pl.multiple_of(fb * 64 + sb * 32 + b * 16, 16), 16)
        o = own[sub, :]
        oshard[b * 16:(b + 1) * 16, :] = o
        v = o + rmine[b * 16:(b + 1) * 16, :]
        scale = lax.rsqrt(jnp.mean(v * v, axis=-1, keepdims=True) + 1e-5)
        h[pl.ds(pl.multiple_of(row0 + b * 16, 16), 16), :] = (v * scale * norm_w[...]).astype(BF16)
    for c in wcopies:
        c.wait()
    per = CW // KD
    all_gather(where, h, gsem, lambda c: proj_steps(c * per, (c + 1) * per, 0, acc, h, w))
    small[0].wait()
    small[1].wait()
    in_tail(where, acc, h, w, cs, conv_w, conv_b, wx, x, xc, z, p, ptx, prx, psem)


def last_kernel(yg, w_out, oshard, out, wout, own, tx0, rx0, tx1, rx1, tx2, rx2, total, osem, rsem, gsem, csem):
    where = place()
    core, fb, sb, partner, first, second = where
    await_peers = enter((partner, first, second))
    ocopies = w_out_copies(1, w_out, wout, osem)
    for c in ocopies:
        c.start()
    reduce_scatter(where, await_peers, yg, wout, ocopies, own, tx0, rx0, tx1, rx1, tx2, rx2, rsem)
    row0 = core * 128 + fb * 64 + sb * 32
    for b in range(2):
        sub = pl.ds(pl.multiple_of(fb * 64 + sb * 32 + b * 16, 16), 16)
        total[pl.ds(pl.multiple_of(row0 + b * 16, 16), 16), :] = (own[sub, :] + oshard[b * 16:(b + 1) * 16, :]).astype(BF16)
    outs = [pltpu.make_async_copy(total.at[:, pl.ds(c * CW, CW)], out.at[:, pl.ds(c * CW, CW)], csem.at[c])
            for c in range(NCH)]
    all_gather(where, total, gsem, lambda c: outs[c].start())
    for c in outs:
        c.wait()


NB = 16
TB = TOK // NB


def ssm_kernel(layer, p, x, xc, z, w_dt, b_dt, a_log, d_skip, cs_hbm, st_hbm, *refs):
    if layer:
        refs = refs[2:]
    yg, conv_out, st_out, st, dt_raw, dts, us, ys, a, bc, cs, isem, osem, csem = refs
    ins = [pltpu.make_async_copy(st_hbm.at[layer, pl.ds(i * TB, TB)], st.at[pl.ds(i * TB, TB)], isem.at[i])
           for i in range(NB)]
    for c in ins:
        c.start()
    cin = pltpu.make_async_copy(cs_hbm.at[layer, pl.ds(1, 2)], cs, csem.at[0])
    cin.start()
    a[...] = -jnp.exp(a_log[...])
    for hf in range(2):
        low = p[hf, 0:RANK, :]
        low = low * lax.rsqrt(jnp.mean(low * low, axis=0, keepdims=True) + 1e-6)
        dt_raw[hf * 128:(hf + 1) * 128, :] = lax.dot_general(
            low.astype(BF16), w_dt[...], (((0,), (0,)), ((), ())), preferred_element_type=F32)
        for k in range(2):
            v = p[hf, RANK + k * NST:RANK + (k + 1) * NST, :]
            bc[hf, k * NST:(k + 1) * NST, :] = v * lax.rsqrt(jnp.mean(v * v, axis=0, keepdims=True) + 1e-6)
    cin.wait()
    couts = [pltpu.make_async_copy(cs, conv_out.at[layer, pl.ds(0, 2)], csem.at[1]),
             pltpu.make_async_copy(x, conv_out.at[layer, 2], csem.at[2])]
    for c in couts:
        c.start()

    def block(i, carry):
        r = rows(i * TB, TB)
        pltpu.make_async_copy(st_hbm.at[layer, r], st.at[r], isem.at[i]).wait()
        dt = jax.nn.softplus(dt_raw[r, :] + b_dt[...])
        xf = xc[r, :].astype(F32)
        dts[...] = dt
        us[...] = dt * xf
        hf = lax.div(i, NB // 2)
        shift = lax.rem(128 - lax.rem(i, NB // 2) * TB, 128)
        bct = pltpu.roll(bc[hf], shift, 1)
        for j in range(TB):
            bx = bct[0:NST, j:j + 1]
            cx = bct[NST:2 * NST, j:j + 1]
            s = jnp.exp(dts[j:j + 1, :] * a[...]) * st[i * TB + j] + us[j:j + 1, :] * bx
            st[i * TB + j] = s
            ys[j:j + 1, :] = jnp.sum(s * cx, axis=0, keepdims=True)
        pltpu.make_async_copy(st.at[r], st_out.at[layer, r], osem.at[i]).start()
        zf = z[r, :].astype(F32)
        y = ys[...] + d_skip[...] * xf
        yg[r, :] = (y * (zf * jax.nn.sigmoid(zf))).astype(BF16)
        return carry

    lax.fori_loop(0, NB, block, 0)
    for c in couts:
        c.wait()
    for i in range(NB):
        pltpu.make_async_copy(st.at[pl.ds(i * TB, TB)], st_out.at[layer, pl.ds(i * TB, TB)], osem.at[i]).wait()


def sds(shape, dtype):
    return jax.ShapeDtypeStruct(shape, dtype)


IN_OUTS = (sds((TOK, CH), BF16), sds((TOK, CH), BF16), sds((TOK, CH), BF16), sds((2, PW, 128), F32))
P_SCRATCH = [pltpu.VMEM((4, PW, 128), BF16), pltpu.VMEM((4, PW, 128), BF16)]
RS_SCRATCH = [pltpu.VMEM((CH, DIM), BF16), pltpu.VMEM((128, DIM), F32)] + [
    pltpu.VMEM((n, DIM), BF16) for n in (128, 128, 64, 64, 32, 32)]


def params(collective_id=None, mib=60):
    if collective_id is None:
        return pltpu.CompilerParams(vmem_limit_bytes=mib << 20)
    return pltpu.CompilerParams(vmem_limit_bytes=mib << 20, collective_id=collective_id, has_side_effects=True)


def solution(mesh):
    def first_call(residual, norm_w, w_in, conv_w, conv_b, wx, cs):
        return pl.pallas_call(
            first_kernel, out_shape=IN_OUTS, in_specs=[ANY, VMEM, ANY, VMEM, VMEM, ANY, ANY], out_specs=(VMEM,) * 4,
            scratch_shapes=[pltpu.VMEM((TOK, DIM), BF16), pltpu.VMEM((DIM, 2, CH), BF16), pltpu.VMEM((TOK, CH), F32),
                            pltpu.VMEM((TOK, DIM), F32), pltpu.VMEM((PW, CH), BF16), pltpu.VMEM((3, TOK, CH), BF16),
                            *P_SCRATCH, DMA((NW,)), DMA((10,)), DMA((2, 4))],
            compiler_params=params(0), name="first",
        )(residual, norm_w, w_in, conv_w, conv_b, wx, cs)

    def middle_call(yg, w_out, residual, norm_w, w_in, conv_w, conv_b, wx, cs):
        return pl.pallas_call(
            middle_kernel, out_shape=(*IN_OUTS, sds((32, DIM), F32)),
            in_specs=[VMEM, ANY, ANY, VMEM, ANY, VMEM, VMEM, ANY, ANY], out_specs=(VMEM,) * 5,
            scratch_shapes=[*RS_SCRATCH, pltpu.VMEM((32, DIM), F32),
                            pltpu.VMEM((TOK, DIM), BF16), pltpu.VMEM((DIM, 2, CH), BF16), pltpu.VMEM((TOK, CH), F32),
                            pltpu.VMEM((PW, CH), BF16), pltpu.VMEM((3, TOK, CH), BF16), *P_SCRATCH,
                            DMA((NCH,)), DMA((NW,)), DMA((3,)), DMA((2, 3 * NCH)), DMA((2, 3 * NCH)), DMA((2, 4))],
            compiler_params=params(1), name="middle",
        )(yg, w_out, residual, norm_w, w_in, conv_w, conv_b, wx, cs)

    def last_call(yg, w_out, oshard):
        return pl.pallas_call(
            last_kernel, out_shape=sds((TOK, DIM), BF16), in_specs=[VMEM, ANY, VMEM], out_specs=ANY,
            scratch_shapes=[*RS_SCRATCH, pltpu.VMEM((TOK, DIM), BF16),
                            DMA((NCH,)), DMA((2, 3 * NCH)), DMA((2, 3 * NCH)), DMA((NCH,))],
            compiler_params=params(2), name="last",
        )(yg, w_out, oshard)

    def ssm_call(layer, p, x, xc, z, w_dt, b_dt, a_log, d_skip, cs, st, held=()):
        return pl.pallas_call(
            functools.partial(ssm_kernel, layer),
            out_shape=(sds((TOK, CH), BF16), sds(cs.shape, BF16), sds(st.shape, F32)),
            in_specs=[VMEM] * 8 + [ANY, ANY] + [ANY] * len(held), out_specs=(VMEM, ANY, ANY),
            input_output_aliases={10: 1, 11: 2} if held else {},
            scratch_shapes=[pltpu.VMEM((TOK, NST, CH), F32), pltpu.VMEM((TOK, CH), F32), pltpu.VMEM((TB, CH), F32),
                            pltpu.VMEM((TB, CH), F32), pltpu.VMEM((TB, CH), F32), pltpu.VMEM((NST, CH), F32),
                            pltpu.VMEM((2, 2 * NST, 128), F32), pltpu.VMEM((2, TOK, CH), BF16),
                            DMA((NB,)), DMA((NB,)), DMA((3,))],
            compiler_params=params(), name=f"ssm{layer}",
        )(p, x, xc, z, w_dt, b_dt, a_log, d_skip, cs, st, *held)

    def device_step(residual, norm_w, w_in, conv_w, conv_b, w_x, w_dt, b_dt, a_log, d_skip, w_out, conv_state, ssm_state):
        cs = jnp.swapaxes(conv_state, 1, 2)
        wx = jnp.swapaxes(w_x, 1, 2)
        norm_w, conv_w, conv_b = norm_w.astype(F32), conv_w.astype(F32), conv_b.astype(F32)

        def conv_args(layer):
            return norm_w[layer:layer + 1], w_in, conv_w[layer], conv_b[layer:layer + 1], wx, cs

        def ssm_args(layer):
            return w_dt[layer], b_dt[layer:layer + 1], a_log[layer], d_skip[layer:layer + 1], cs, ssm_state

        x, xc, z, p = first_call(residual, *conv_args(0))
        yg, conv_out, ssm_out = ssm_call(0, p, x, xc, z, *ssm_args(0))
        x, xc, z, p, oshard = middle_call(yg, w_out, residual, *conv_args(1))
        yg, conv_out, ssm_out = ssm_call(1, p, x, xc, z, *ssm_args(1), (conv_out, ssm_out))
        total = last_call(yg, w_out, oshard)
        return residual + total.astype(F32), jnp.swapaxes(conv_out, 1, 2), ssm_out

    cache_spec = P(None, 'dp', None, 'tp')
    in_specs = (P('dp', None), P(None, None), P(None, None, None, 'tp'), P(None, None, 'tp'), P(None, 'tp'), P(None, 'tp', None), P(None, None, 'tp'), P(None, 'tp'), P(None, None, 'tp'), P(None, 'tp'), P(None, 'tp', None), cache_spec, cache_spec)
    out_specs = (P('dp', None), cache_spec, cache_spec)
    return jax.shard_map(device_step, mesh=mesh, in_specs=in_specs, out_specs=out_specs, check_vma=False)
```

```python
import functools

import jax
import jax.numpy as jnp
from jax import lax
from jax.experimental import pallas as pl
from jax.experimental.pallas import tpu as pltpu
from jax.sharding import PartitionSpec as P

F32 = jnp.float32
BF16 = jnp.bfloat16
MESH = pl.DeviceIdType.MESH
VMEM = pl.BlockSpec(memory_space=pltpu.VMEM)
ANY = pl.BlockSpec(memory_space=pltpu.HBM)
DMA = pltpu.SemaphoreType.DMA

TOK = 256
DIM = 4096
CH = 1024
PW = 288
NST = 16
RANK = 256
NCH = 4
CW = DIM // NCH
NW = 8
KD = 256
NB = 16
TB = TOK // NB
AHEAD = (NB, 9)


def rows(start, size):
    return pl.ds(pl.multiple_of(start, size), size)


def place():
    me = lax.axis_index("tp")
    core = lax.rem(me, 2)
    xb = lax.rem(lax.div(me, 2), 2)
    yb = lax.div(me, 4)
    partner = me + 1 - 2 * core
    xn = me + 2 - 4 * xb
    yn = me + 4 - 8 * yb
    first = xn * (1 - core) + yn * core
    second = yn * (1 - core) + xn * core
    fb = xb * (1 - core) + yb * core
    sb = yb * (1 - core) + xb * core
    return core, fb, sb, partner, first, second


def enter(peers):
    barrier = pltpu.get_barrier_semaphore()
    for peer in peers:
        pl.semaphore_signal(barrier, inc=1, device_id={"tp": peer}, device_id_type=MESH)
    return lambda: pl.semaphore_wait(barrier, len(peers))


def remote(src, dst, sems, idx, to):
    return pltpu.make_async_remote_copy(
        src_ref=src, dst_ref=dst, send_sem=sems.at[0, idx], recv_sem=sems.at[1, idx],
        device_id={"tp": to}, device_id_type=MESH)


def spread(parity):
    src = lax.broadcasted_iota(jnp.int32, (128, 256), 0)
    dst = lax.broadcasted_iota(jnp.int32, (128, 256), 1)
    return jnp.where(dst == 2 * src + parity, 1.0, 0.0).astype(BF16)


def proj_steps(lo, hi, parity, acc, h, w):
    sel = spread(parity)

    def step(i, carry):
        cols = rows(i * KD, KD)
        hc = h[:, cols]
        lhs = jnp.concatenate(
            [jnp.dot(hc[:, j * 128:(j + 1) * 128], sel, preferred_element_type=F32).astype(BF16)
             for j in range(KD // 128)], axis=1)
        wc = w[cols, :, 0:CH].reshape(2 * KD, CH)
        acc[...] += jnp.dot(lhs, wc, preferred_element_type=F32)
        return carry

    lax.fori_loop(lo, hi, step, 0)


def copies(pairs, sem):
    return [pltpu.make_async_copy(src, dst, sem.at[i]) for i, (src, dst) in enumerate(pairs)]


def start(group):
    for c in group:
        c.start()


def wait(group):
    for c in group:
        c.wait()


def w_in_copies(layer, w_in, w, sem):
    size = DIM // NW
    return copies([(w_in.at[layer, pl.ds(i * size, size)], w.at[pl.ds(i * size, size), :, pl.ds(0, CH)])
                   for i in range(NW)], sem)


def state_copies(layer, st, dst, sem, lo=0, hi=None):
    hi = AHEAD[layer] if hi is None else hi
    return copies([(st.at[layer, pl.ds(i * TB, TB)], dst.at[pl.ds(i * TB, TB)]) for i in range(lo, hi)], sem)


def conv_stage(layer, acc, cs, cwb, cbb, cw, cb, x, xc):
    cw[...] = cwb[layer].astype(F32)
    cb[...] = cbb[layer:layer + 1, :].astype(F32)

    def block(i, carry):
        r = rows(i * 32, 32)
        xv = acc[r, :].astype(BF16)
        x[r, :] = xv
        pre = cs[0, r, :].astype(F32) * cw[0:1, :]
        pre += cs[1, r, :].astype(F32) * cw[1:2, :]
        pre += cs[2, r, :].astype(F32) * cw[2:3, :]
        pre += xv.astype(F32) * cw[3:4, :]
        pre += cb[...]
        xc[r, :] = (pre * jax.nn.sigmoid(pre)).astype(BF16)
        return carry

    lax.fori_loop(0, TOK // 32, block, 0)


def p_stage(where, z_part, xc, wx, p, ptx, prx, psem):
    core, _, _, partner, first, second = where

    def half(index):
        return lax.dot_general(wx[...], xc[rows(index * 128, 128), :], (((1,), (1,)), ((), ())),
                               preferred_element_type=F32)

    ptx[0] = half(1 - core).astype(BF16)
    hop = remote(ptx.at[0], prx.at[0], psem, 0, partner)
    hop.start()
    p[core] = half(core)
    z_part(0)
    hop.wait()
    for k, to in ((1, first), (2, second), (3, partner)):
        p[core] += prx[k - 1].astype(F32)
        ptx[k] = p[core].astype(BF16)
        hop = remote(ptx.at[k], prx.at[k], psem, k, to)
        hop.start()
        z_part(k)
        hop.wait()
    p[1 - core] = prx[3].astype(F32)


def in_tail(layer, where, acc, h, w, cs, conv, wx, x, xc, z, p, ptx, prx, psem):
    conv_stage(layer, acc, cs, *conv, x, xc)
    acc[...] = jnp.zeros_like(acc)
    n = DIM // KD
    cuts = (0, n // 8, n // 2, n - n // 8, n)

    def z_part(k):
        proj_steps(cuts[k], cuts[k + 1], 1, acc, h, w)

    p_stage(where, z_part, xc, wx, p, ptx, prx, psem)

    def block(i, carry):
        r = rows(i * 32, 32)
        z[r, :] = acc[r, :].astype(BF16)
        return carry

    lax.fori_loop(0, TOK // 32, block, 0)


def first_kernel(resid, nw_hbm, w_in, cw_hbm, cb_hbm, wx_hbm, cs_hbm, st_hbm, x, xc, z, p, cs, st,
                 h, w, acc, rbuf, wx, nwb, nw, cwb, cbb, cw, cb, ptx, prx, wsem, rsem, lsem, ssem, psem):
    where = place()
    core, fb, sb, partner, first, second = where
    await_peers = enter((partner, first, second))
    small = copies([(nw_hbm, nwb), (cw_hbm, cwb), (cb_hbm, cbb), (wx_hbm.at[0], wx), (cs_hbm.at[0], cs)], lsem)
    small[0].start()
    nr = 8
    start(copies([(resid.at[pl.ds(i * 32, 32)], rbuf.at[pl.ds(i * 32, 32)]) for i in range(nr)], rsem))
    wcopies = w_in_copies(0, w_in, w, wsem)
    start(wcopies)
    start(small[1:])
    acc[...] = jnp.zeros_like(acc)
    small[0].wait()
    nw[...] = nwb[0:1, :].astype(F32)

    def norm_block(i, carry):
        pltpu.make_async_copy(resid.at[rows(i * 32, 32)], rbuf.at[rows(i * 32, 32)], rsem.at[i]).wait()
        for b in range(2):
            r = pl.ds(pl.multiple_of(i * 32 + b * 16, 16), 16)
            v = rbuf[r, :]
            scale = lax.rsqrt(jnp.mean(v * v, axis=-1, keepdims=True) + 1e-5)
            h[r, :] = (v * scale * nw[...]).astype(BF16)
        return carry

    lax.fori_loop(0, nr, norm_block, 0)
    per = DIM // NW // KD
    for i in range(NW):
        wcopies[i].wait()
        proj_steps(i * per, (i + 1) * per, 0, acc, h, w)
    scopies = state_copies(0, st_hbm, st, ssem)
    start(scopies)
    wait(small[1:])
    await_peers()
    in_tail(0, where, acc, h, w, cs, (cwb, cbb, cw, cb), wx, x, xc, z, p, ptx, prx, psem)
    wait(scopies)


def w_out_copies(layer, w_out, wout, sem):
    return copies([(w_out.at[layer, :, pl.ds(c * CW, CW)], wout.at[:, pl.ds(c * CW, CW)]) for c in range(NCH)], sem)


def reduce_scatter(where, await_peers, yg, wout, wcopies, own, tx0, rx0, tx1, rx1, tx2, rx2, rsem):
    core, fb, sb, partner, first, second = where
    col = [pl.ds(c * CW, CW) for c in range(NCH)]
    hop0 = [remote(tx0.at[:, col[c]], rx0.at[:, col[c]], rsem, c, partner) for c in range(NCH)]
    hop1 = [remote(tx1.at[:, col[c]], rx1.at[:, col[c]], rsem, NCH + c, first) for c in range(NCH)]
    hop2 = [remote(tx2.at[:, col[c]], rx2.at[:, col[c]], rsem, 2 * NCH + c, second) for c in range(NCH)]

    def product(c):
        wcopies[c].wait()
        wc = wout[:, col[c]]
        tx0[:, col[c]] = jnp.dot(yg[rows((1 - core) * 128, 128), :], wc, preferred_element_type=F32).astype(BF16)
        if c == 0:
            await_peers()
        hop0[c].start()
        own[:, col[c]] = jnp.dot(yg[rows(core * 128, 128), :], wc, preferred_element_type=F32)

    def stage1(c):
        hop0[c].wait()
        give, keep = rows((1 - fb) * 64, 64), rows(fb * 64, 64)
        tx1[:, col[c]] = (own[give, col[c]] + rx0[give, col[c]].astype(F32)).astype(BF16)
        hop1[c].start()
        own[keep, col[c]] += rx0[keep, col[c]].astype(F32)

    def stage2(c):
        hop1[c].wait()
        give, keep = (1 - sb) * 32, sb * 32
        tx2[:, col[c]] = (own[rows(fb * 64 + give, 32), col[c]] + rx1[rows(give, 32), col[c]].astype(F32)).astype(BF16)
        hop2[c].start()
        own[rows(fb * 64 + keep, 32), col[c]] += rx1[rows(keep, 32), col[c]].astype(F32)

    product(0)
    product(1)
    stage1(0)
    product(2)
    stage1(1)
    product(3)
    stage1(2)
    stage1(3)
    for c in range(NCH):
        stage2(c)
    mine = rows(fb * 64 + sb * 32, 32)
    for c in range(NCH):
        hop2[c].wait()
        own[mine, col[c]] += rx2[:, col[c]].astype(F32)


def all_gather(where, h, gsem, consume):
    core, fb, sb, partner, first, second = where
    col = [pl.ds(c * CW, CW) for c in range(NCH)]
    base = core * 128

    def hops(k, begin, size, to):
        part = [h.at[rows(begin, size), col[c]] for c in range(NCH)]
        return [remote(part[c], part[c], gsem, k * NCH + c, to) for c in range(NCH)]

    hop0 = hops(0, base + fb * 64 + sb * 32, 32, second)
    hop1 = hops(1, base + fb * 64, 64, first)
    hop2 = hops(2, base, 128, partner)
    for c in range(NCH):
        hop0[c].start()
    for c in range(NCH):
        hop0[c].wait()
        hop1[c].start()
    for c in range(NCH):
        hop1[c].wait()
        hop2[c].start()
    for c in range(NCH):
        hop2[c].wait()
        consume(c)


def my_rows(where):
    core, fb, sb = where[:3]
    for b in range(2):
        off = fb * 64 + sb * 32 + b * 16
        yield pl.ds(pl.multiple_of(off, 16), 16), pl.ds(pl.multiple_of(core * 128 + off, 16), 16), pl.ds(b * 16, 16)


def middle_kernel(yg, w_out, resid, nw_hbm, w_in, cw_hbm, cb_hbm, wx_hbm, cs_hbm, st_hbm,
                  x, xc, z, p, cs, st, oshard,
                  wout, own, tx0, rx0, tx1, rx1, tx2, rx2, rmine,
                  h, w, acc, wx, nwb, nw, cwb, cbb, cw, cb, ptx, prx, osem, wsem, lsem, ssem, rsem, gsem, psem):
    where = place()
    core, fb, sb, partner, first, second = where
    await_peers = enter((partner, first, second))
    ocopies = w_out_copies(0, w_out, wout, osem)
    start(ocopies)
    row0 = core * 128 + fb * 64 + sb * 32
    small = copies([(nw_hbm, nwb), (cw_hbm, cwb), (cb_hbm, cbb), (wx_hbm.at[1], wx), (cs_hbm.at[1], cs),
                    (resid.at[rows(row0, 32)], rmine)], lsem)
    start(small)
    wcopies = w_in_copies(1, w_in, w, wsem)
    start(wcopies)
    reduce_scatter(where, await_peers, yg, wout, ocopies, own, tx0, rx0, tx1, rx1, tx2, rx2, rsem)
    wait(small)
    nw[...] = nwb[1:2, :].astype(F32)
    for sub, whole, part in my_rows(where):
        o = own[sub, :]
        oshard[part, :] = o
        v = o + rmine[part, :]
        scale = lax.rsqrt(jnp.mean(v * v, axis=-1, keepdims=True) + 1e-5)
        h[whole, :] = (v * scale * nw[...]).astype(BF16)
    wait(wcopies)
    scopies = state_copies(1, st_hbm, st, ssem)
    start(scopies)
    acc[...] = jnp.zeros_like(acc)
    per = CW // KD
    all_gather(where, h, gsem, lambda c: proj_steps(c * per, (c + 1) * per, 0, acc, h, w))
    in_tail(1, where, acc, h, w, cs, (cwb, cbb, cw, cb), wx, x, xc, z, p, ptx, prx, psem)
    wait(scopies)


def last_kernel(yg, oshard, w_out, resid, out, wout, own, tx0, rx0, tx1, rx1, tx2, rx2, total, rbuf, osem, lsem, rsem, gsem):
    where = place()
    core, fb, sb, partner, first, second = where
    await_peers = enter((partner, first, second))
    ocopies = w_out_copies(1, w_out, wout, osem)
    start(ocopies)
    rcopy = pltpu.make_async_copy(resid, rbuf, lsem.at[0])
    rcopy.start()
    reduce_scatter(where, await_peers, yg, wout, ocopies, own, tx0, rx0, tx1, rx1, tx2, rx2, rsem)
    for sub, whole, part in my_rows(where):
        total[whole, :] = (own[sub, :] + oshard[part, :]).astype(BF16)
    rcopy.wait()

    def consume(c):
        col = pl.ds(c * CW, CW)

        def block(i, carry):
            r = rows(i * 32, 32)
            out[r, col] = rbuf[r, col] + total[r, col].astype(F32)
            return carry

        lax.fori_loop(0, TOK // 32, block, 0)

    all_gather(where, total, gsem, consume)


def ssm_kernel(layer, x, xc, z, p, cs, st, wdt_hbm, bdt_hbm, alog_hbm, dskip_hbm, st_hbm, *refs):
    if layer:
        refs = refs[2:]
    yg, conv_out, st_out, new, dt_raw, dts, us, ys, a, bc, wdt, bdt, dskip, bdt1, dskip1, lsem, osem, csem, isem = refs
    small = copies([(bdt_hbm, bdt), (dskip_hbm, dskip), (alog_hbm.at[layer], a), (wdt_hbm.at[layer], wdt)], lsem)
    start(small)
    ahead = AHEAD[layer]
    start(state_copies(layer, st_hbm, new, isem, ahead, NB))
    couts = copies([(cs.at[pl.ds(1, 2)], conv_out.at[layer, pl.ds(0, 2)]), (x, conv_out.at[layer, 2])], csem)
    start(couts)
    for hf in range(2):
        for k in range(2):
            v = p[hf, RANK + k * NST:RANK + (k + 1) * NST, :]
            bc[hf, k * NST:(k + 1) * NST, :] = v * lax.rsqrt(jnp.mean(v * v, axis=0, keepdims=True) + 1e-6)
    wait(small)
    a[...] = -jnp.exp(a[...])
    bdt1[...] = bdt[layer:layer + 1, :]
    dskip1[...] = dskip[layer:layer + 1, :]
    for hf in range(2):
        low = p[hf, 0:RANK, :]
        low = low * lax.rsqrt(jnp.mean(low * low, axis=0, keepdims=True) + 1e-6)
        dt_raw[hf * 128:(hf + 1) * 128, :] = lax.dot_general(
            low.astype(BF16), wdt[...], (((0,), (0,)), ((), ())), preferred_element_type=F32)

    def out_copy(i):
        r = rows(i * TB, TB)
        return pltpu.make_async_copy(new.at[r], st_out.at[layer, r], osem.at[i])

    def block(src, i, carry):
        r = rows(i * TB, TB)
        if src is new:
            pltpu.make_async_copy(st_hbm.at[layer, r], new.at[r], isem.at[i - ahead]).wait()
        dt = jax.nn.softplus(dt_raw[r, :] + bdt1[...])
        xf = xc[r, :].astype(F32)
        dts[...] = dt
        us[...] = dt * xf
        hf = lax.div(i, NB // 2)
        shift = lax.rem(128 - lax.rem(i, NB // 2) * TB, 128)
        bct = pltpu.roll(bc[hf], shift, 1)
        for j in range(TB):
            bx = bct[0:NST, j:j + 1]
            cx = bct[NST:2 * NST, j:j + 1]
            s = jnp.exp(dts[j:j + 1, :] * a[...]) * src[i * TB + j] + us[j:j + 1, :] * bx
            new[i * TB + j] = s
            ys[j:j + 1, :] = jnp.sum(s * cx, axis=0, keepdims=True)
        out_copy(i).start()
        zf = z[r, :].astype(F32)
        y = ys[...] + dskip1[...] * xf
        yg[r, :] = (y * (zf * jax.nn.sigmoid(zf))).astype(BF16)
        return carry

    lax.fori_loop(0, ahead, functools.partial(block, st), 0)
    if ahead < NB:
        lax.fori_loop(ahead, NB, functools.partial(block, new), 0)
    wait(couts)
    for i in range(NB):
        out_copy(i).wait()


def sds(shape, dtype):
    return jax.ShapeDtypeStruct(shape, dtype)


def in_outs(layer):
    return (pltpu.VMEM((TOK, CH), BF16),) * 3 + (
        pltpu.VMEM((2, PW, 128), F32), pltpu.VMEM((3, TOK, CH), BF16), pltpu.VMEM((AHEAD[layer] * TB, NST, CH), F32))


PROJ_SCRATCH = [pltpu.VMEM((TOK, DIM), BF16), pltpu.VMEM((DIM, 2, CH + 128), BF16), pltpu.VMEM((TOK, CH), F32)]
P_SCRATCH = [pltpu.VMEM((PW, CH), BF16), pltpu.VMEM((2, DIM), BF16), pltpu.VMEM((1, DIM), F32),
             pltpu.VMEM((2, 4, CH), BF16), pltpu.VMEM((2, CH), BF16), pltpu.VMEM((4, CH), F32), pltpu.VMEM((1, CH), F32),
             pltpu.VMEM((4, PW, 128), BF16), pltpu.VMEM((4, PW, 128), BF16)]
RS_SCRATCH = [pltpu.VMEM((CH, DIM), BF16), pltpu.VMEM((128, DIM), F32)] + [pltpu.VMEM((n, DIM), BF16) for n in (128, 128, 64, 64, 32, 32)]


def params(mib, collective_id=None):
    if collective_id is None:
        return pltpu.CompilerParams(vmem_limit_bytes=mib << 20)
    return pltpu.CompilerParams(vmem_limit_bytes=mib << 20, collective_id=collective_id, has_side_effects=True)


def solution(mesh):
    def first_call(residual, *args):
        return pl.pallas_call(
            first_kernel, out_shape=in_outs(0), in_specs=[ANY] * 8, out_specs=(VMEM,) * 6,
            scratch_shapes=[*PROJ_SCRATCH, pltpu.VMEM((TOK, DIM), F32), *P_SCRATCH,
                            DMA((NW,)), DMA((8,)), DMA((5,)), DMA((NB,)), DMA((2, 4))],
            compiler_params=params(34, 0), name="first",
        )(residual, *args)

    def middle_call(yg, w_out, residual, *args):
        return pl.pallas_call(
            middle_kernel, out_shape=(*in_outs(1), pltpu.VMEM((32, DIM), F32)),
            in_specs=[VMEM] + [ANY] * 9, out_specs=(VMEM,) * 7,
            scratch_shapes=[*RS_SCRATCH, pltpu.VMEM((32, DIM), F32), *PROJ_SCRATCH, *P_SCRATCH,
                            DMA((NCH,)), DMA((NW,)), DMA((6,)), DMA((NB,)), DMA((2, 3 * NCH)), DMA((2, 3 * NCH)), DMA((2, 4))],
            compiler_params=params(47, 1), name="middle",
        )(yg, w_out, residual, *args)

    def last_call(yg, oshard, w_out, residual):
        return pl.pallas_call(
            last_kernel, out_shape=pltpu.VMEM((TOK, DIM), F32), in_specs=[VMEM, VMEM, ANY, ANY], out_specs=VMEM,
            scratch_shapes=[*RS_SCRATCH, pltpu.VMEM((TOK, DIM), BF16), pltpu.VMEM((TOK, DIM), F32),
                            DMA((NCH,)), DMA((1,)), DMA((2, 3 * NCH)), DMA((2, 3 * NCH))],
            compiler_params=params(56, 2), name="last",
        )(yg, oshard, w_out, residual)

    def ssm_call(layer, held, shapes, *args):
        return pl.pallas_call(
            functools.partial(ssm_kernel, layer),
            out_shape=(pltpu.VMEM((TOK, CH), BF16), *shapes),
            in_specs=[VMEM] * 6 + [ANY] * (5 + len(held)), out_specs=(VMEM, ANY, ANY),
            input_output_aliases={11: 1, 12: 2} if held else {},
            scratch_shapes=[pltpu.VMEM((TOK, NST, CH), F32), pltpu.VMEM((TOK, CH), F32), pltpu.VMEM((TB, CH), F32),
                            pltpu.VMEM((TB, CH), F32), pltpu.VMEM((TB, CH), F32), pltpu.VMEM((NST, CH), F32),
                            pltpu.VMEM((2, 2 * NST, 128), F32), pltpu.VMEM((RANK, CH), BF16),
                            pltpu.VMEM((2, CH), F32), pltpu.VMEM((2, CH), F32), pltpu.VMEM((1, CH), F32), pltpu.VMEM((1, CH), F32),
                            DMA((4,)), DMA((NB,)), DMA((2,)), DMA((NB,))],
            compiler_params=params(24), name=f"ssm{layer}",
        )(*args, *held)

    def device_step(residual, norm_w, w_in, conv_w, conv_b, w_x, w_dt, b_dt, a_log, d_skip, w_out, conv_state, ssm_state):
        cs = jnp.swapaxes(conv_state, 1, 2)
        wx = jnp.swapaxes(w_x, 1, 2)
        shapes = (sds(cs.shape, BF16), sds(ssm_state.shape, F32))
        in_args = (residual, norm_w, w_in, conv_w, conv_b, wx, cs, ssm_state)
        ssm_args = (w_dt, b_dt, a_log, d_skip, ssm_state)
        yg, *held = ssm_call(0, (), shapes, *first_call(*in_args), *ssm_args)
        *mid, oshard = middle_call(yg, w_out, *in_args)
        yg, conv_out, ssm_out = ssm_call(1, tuple(held), shapes, *mid, *ssm_args)
        return last_call(yg, oshard, w_out, residual), jnp.swapaxes(conv_out, 1, 2), ssm_out

    cache_spec = P(None, 'dp', None, 'tp')
    in_specs = (P('dp', None), P(None, None), P(None, None, None, 'tp'), P(None, None, 'tp'), P(None, 'tp'), P(None, 'tp', None), P(None, None, 'tp'), P(None, 'tp'), P(None, None, 'tp'), P(None, 'tp'), P(None, 'tp', None), cache_spec, cache_spec)
    out_specs = (P('dp', None), cache_spec, cache_spec)
    return jax.shard_map(device_step, mesh=mesh, in_specs=in_specs, out_specs=out_specs, check_vma=False)
```

```python
import functools

import jax
import jax.numpy as jnp
from jax import lax
from jax.experimental import pallas as pl
from jax.experimental.pallas import tpu as pltpu
from jax.sharding import PartitionSpec as P

F32 = jnp.float32
BF16 = jnp.bfloat16
MESH = pl.DeviceIdType.MESH
VMEM = pl.BlockSpec(memory_space=pltpu.VMEM)
ANY = pl.BlockSpec(memory_space=pltpu.HBM)
DMA = pltpu.SemaphoreType.DMA

TOK = 256
DIM = 4096
CH = 1024
PW = 288
NST = 16
RANK = 256
NCH = 4
CW = DIM // NCH
NW = 8
KD = 256
NB = 16
TB = TOK // NB
AHEAD = (NB, 8)


def rows(start, size):
    return pl.ds(pl.multiple_of(start, size), size)


def place():
    me = lax.axis_index("tp")
    core = lax.rem(me, 2)
    xb = lax.rem(lax.div(me, 2), 2)
    yb = lax.div(me, 4)
    partner = me + 1 - 2 * core
    xn = me + 2 - 4 * xb
    yn = me + 4 - 8 * yb
    first = xn * (1 - core) + yn * core
    second = yn * (1 - core) + xn * core
    fb = xb * (1 - core) + yb * core
    sb = yb * (1 - core) + xb * core
    return core, fb, sb, partner, first, second


def enter(peers):
    barrier = pltpu.get_barrier_semaphore()
    for peer in peers:
        pl.semaphore_signal(barrier, inc=1, device_id={"tp": peer}, device_id_type=MESH)
    return lambda: pl.semaphore_wait(barrier, len(peers))


def remote(src, dst, sems, idx, to):
    return pltpu.make_async_remote_copy(
        src_ref=src, dst_ref=dst, send_sem=sems.at[0, idx], recv_sem=sems.at[1, idx],
        device_id={"tp": to}, device_id_type=MESH)


def spread(parity):
    src = lax.broadcasted_iota(jnp.int32, (128, 256), 0)
    dst = lax.broadcasted_iota(jnp.int32, (128, 256), 1)
    return jnp.where(dst == 2 * src + parity, 1.0, 0.0).astype(BF16)


def proj_steps(lo, hi, parity, acc, h, w):
    sel = spread(parity)

    def step(i, carry):
        cols = rows(i * KD, KD)
        hc = h[:, cols]
        lhs = jnp.concatenate(
            [jnp.dot(hc[:, j * 128:(j + 1) * 128], sel, preferred_element_type=F32).astype(BF16)
             for j in range(KD // 128)], axis=1)
        wc = w[rows(i * 2 * KD, 2 * KD), :]
        acc[...] += jnp.dot(lhs, wc, preferred_element_type=F32)
        return carry

    lax.fori_loop(lo, hi, step, 0)


def copies(pairs, sem):
    return [pltpu.make_async_copy(src, dst, sem.at[i]) for i, (src, dst) in enumerate(pairs)]


def start(group):
    for c in group:
        c.start()


def wait(group):
    for c in group:
        c.wait()


class WeightStream:
    def __init__(self, layer, w_in, raw, w, sem):
        self.raw, self.w, self.slots = raw, w, raw.shape[0]
        self.size = DIM // NW
        self.copy = [pltpu.make_async_copy(w_in.at[layer, pl.ds(i * self.size, self.size)], raw.at[i % self.slots], sem.at[i])
                     for i in range(NW)]

    def begin(self):
        start(self.copy[:self.slots])

    def lay_out(self, i):
        self.copy[i].wait()
        raw, w, slot, base = self.raw, self.w, i % self.slots, i * self.size

        def block(k, carry):
            w[rows(base * 2 + k * 256, 256), :] = raw[slot, rows(k * 128, 128)].reshape(256, CH)
            return carry

        lax.fori_loop(0, self.size // 128, block, 0)
        if i + self.slots < NW:
            self.copy[i + self.slots].start()


def state_copies(layer, st, dst, sem, lo=0, hi=None):
    hi = AHEAD[layer] if hi is None else hi
    return copies([(st.at[layer, pl.ds(i * TB, TB)], dst.at[pl.ds(i * TB, TB)]) for i in range(lo, hi)], sem)


def conv_stage(layer, acc, cs, cwb, cbb, cw, cb, x, xc):
    cw[...] = cwb[layer].astype(F32)
    cb[...] = cbb[layer:layer + 1, :].astype(F32)

    def block(i, carry):
        r = rows(i * 32, 32)
        xv = acc[r, :].astype(BF16)
        x[r, :] = xv
        pre = cs[0, r, :].astype(F32) * cw[0:1, :]
        pre += cs[1, r, :].astype(F32) * cw[1:2, :]
        pre += cs[2, r, :].astype(F32) * cw[2:3, :]
        pre += xv.astype(F32) * cw[3:4, :]
        pre += cb[...]
        xc[r, :] = (pre * jax.nn.sigmoid(pre)).astype(BF16)
        return carry

    lax.fori_loop(0, TOK // 32, block, 0)


def p_stage(where, z_part, xc, wx, p, ptx, prx, psem):
    core, _, _, partner, first, second = where

    def half(index):
        return lax.dot_general(wx[...], xc[rows(index * 128, 128), :], (((1,), (1,)), ((), ())),
                               preferred_element_type=F32)

    ptx[0] = half(1 - core).astype(BF16)
    hop = remote(ptx.at[0], prx.at[0], psem, 0, partner)
    hop.start()
    p[core] = half(core)
    z_part(0)
    hop.wait()
    for k, to in ((1, first), (2, second), (3, partner)):
        p[core] += prx[k - 1].astype(F32)
        ptx[k] = p[core].astype(BF16)
        hop = remote(ptx.at[k], prx.at[k], psem, k, to)
        hop.start()
        z_part(k)
        hop.wait()
    p[1 - core] = prx[3].astype(F32)


def in_tail(layer, where, acc, h, w, cs, conv, wx, x, xc, z, p, ptx, prx, psem):
    conv_stage(layer, acc, cs, *conv, x, xc)
    acc[...] = jnp.zeros_like(acc)
    n = DIM // KD
    cuts = (0, n // 8, n // 2, n - n // 8, n)

    def z_part(k):
        proj_steps(cuts[k], cuts[k + 1], 1, acc, h, w)

    p_stage(where, z_part, xc, wx, p, ptx, prx, psem)

    def block(i, carry):
        r = rows(i * 32, 32)
        z[r, :] = acc[r, :].astype(BF16)
        return carry

    lax.fori_loop(0, TOK // 32, block, 0)


def first_kernel(resid, nw_hbm, w_in, cw_hbm, cb_hbm, wx_hbm, cs_hbm, st_hbm, x, xc, z, p, cs, st,
                 h, raw, w, acc, rbuf, wx, nwb, nw, cwb, cbb, cw, cb, ptx, prx, wsem, rsem, lsem, ssem, psem):
    where = place()
    core, fb, sb, partner, first, second = where
    await_peers = enter((partner, first, second))
    small = copies([(nw_hbm, nwb), (cw_hbm, cwb), (cb_hbm, cbb), (wx_hbm.at[0], wx), (cs_hbm.at[0], cs)], lsem)
    small[0].start()
    nr = 8
    start(copies([(resid.at[pl.ds(i * 32, 32)], rbuf.at[pl.ds(i * 32, 32)]) for i in range(nr)], rsem))
    stream = WeightStream(0, w_in, raw, w, wsem)
    stream.begin()
    start(small[1:])
    acc[...] = jnp.zeros_like(acc)
    small[0].wait()
    nw[...] = nwb[0:1, :].astype(F32)

    def norm_block(i, carry):
        pltpu.make_async_copy(resid.at[rows(i * 32, 32)], rbuf.at[rows(i * 32, 32)], rsem.at[i]).wait()
        for b in range(2):
            r = pl.ds(pl.multiple_of(i * 32 + b * 16, 16), 16)
            v = rbuf[r, :]
            scale = lax.rsqrt(jnp.mean(v * v, axis=-1, keepdims=True) + 1e-5)
            h[r, :] = (v * scale * nw[...]).astype(BF16)
        return carry

    lax.fori_loop(0, nr, norm_block, 0)
    per = DIM // NW // KD
    for i in range(NW):
        stream.lay_out(i)
        proj_steps(i * per, (i + 1) * per, 0, acc, h, w)
    scopies = state_copies(0, st_hbm, st, ssem)
    start(scopies)
    wait(small[1:])
    await_peers()
    in_tail(0, where, acc, h, w, cs, (cwb, cbb, cw, cb), wx, x, xc, z, p, ptx, prx, psem)
    wait(scopies)


def w_out_copies(layer, w_out, wout, sem):
    return copies([(w_out.at[layer, :, pl.ds(c * CW, CW)], wout.at[:, pl.ds(c * CW, CW)]) for c in range(NCH)], sem)


def reduce_scatter(where, await_peers, yg, wout, wcopies, own, tx0, rx0, tx1, rx1, tx2, rx2, rsem, loads, fill):
    core, fb, sb, partner, first, second = where
    col = [pl.ds(c * CW, CW) for c in range(NCH)]
    hop0 = [remote(tx0.at[:, col[c]], rx0.at[:, col[c]], rsem, c, partner) for c in range(NCH)]
    hop1 = [remote(tx1.at[:, col[c]], rx1.at[:, col[c]], rsem, NCH + c, first) for c in range(NCH)]
    hop2 = [remote(tx2.at[:, col[c]], rx2.at[:, col[c]], rsem, 2 * NCH + c, second) for c in range(NCH)]

    def product(c):
        wcopies[c].wait()
        wc = wout[:, col[c]]
        tx0[:, col[c]] = jnp.dot(yg[rows((1 - core) * 128, 128), :], wc, preferred_element_type=F32).astype(BF16)
        if c == 0:
            await_peers()
        hop0[c].start()
        own[:, col[c]] = jnp.dot(yg[rows(core * 128, 128), :], wc, preferred_element_type=F32)

    def stage1(c):
        hop0[c].wait()
        give, keep = rows((1 - fb) * 64, 64), rows(fb * 64, 64)
        tx1[:, col[c]] = (own[give, col[c]] + rx0[give, col[c]].astype(F32)).astype(BF16)
        hop1[c].start()
        own[keep, col[c]] += rx0[keep, col[c]].astype(F32)

    def stage2(c):
        hop1[c].wait()
        give, keep = (1 - sb) * 32, sb * 32
        tx2[:, col[c]] = (own[rows(fb * 64 + give, 32), col[c]] + rx1[rows(give, 32), col[c]].astype(F32)).astype(BF16)
        hop2[c].start()
        own[rows(fb * 64 + keep, 32), col[c]] += rx1[rows(keep, 32), col[c]].astype(F32)

    product(0)
    product(1)
    stage1(0)
    product(2)
    stage1(1)
    product(3)
    loads()
    stage1(2)
    stage1(3)
    fill()
    fill()
    for c in range(NCH):
        stage2(c)
        fill()
    fill()
    fill()
    mine = rows(fb * 64 + sb * 32, 32)
    for c in range(NCH):
        hop2[c].wait()
        own[mine, col[c]] += rx2[:, col[c]].astype(F32)


def all_gather(where, h, gsem, consume):
    core, fb, sb, partner, first, second = where
    col = [pl.ds(c * CW, CW) for c in range(NCH)]
    base = core * 128

    def hops(k, begin, size, to):
        part = [h.at[rows(begin, size), col[c]] for c in range(NCH)]
        return [remote(part[c], part[c], gsem, k * NCH + c, to) for c in range(NCH)]

    hop0 = hops(0, base + fb * 64 + sb * 32, 32, second)
    hop1 = hops(1, base + fb * 64, 64, first)
    hop2 = hops(2, base, 128, partner)
    for c in range(NCH):
        hop0[c].start()
    for c in range(NCH):
        hop0[c].wait()
        hop1[c].start()
    for c in range(NCH):
        hop1[c].wait()
        hop2[c].start()
    for c in range(NCH):
        hop2[c].wait()
        consume(c)


def my_rows(where):
    core, fb, sb = where[:3]
    for b in range(2):
        off = fb * 64 + sb * 32 + b * 16
        yield pl.ds(pl.multiple_of(off, 16), 16), pl.ds(pl.multiple_of(core * 128 + off, 16), 16), pl.ds(b * 16, 16)


def middle_kernel(yg, w_out, resid, nw_hbm, w_in, cw_hbm, cb_hbm, wx_hbm, cs_hbm, st_hbm,
                  x, xc, z, p, cs, st, oshard,
                  wout, own, tx0, rx0, tx1, rx1, tx2, rx2, rmine,
                  h, raw, w, acc, wx, nwb, nw, cwb, cbb, cw, cb, ptx, prx, osem, wsem, lsem, ssem, rsem, gsem, psem):
    where = place()
    core, fb, sb, partner, first, second = where
    await_peers = enter((partner, first, second))
    ocopies = w_out_copies(0, w_out, wout, osem)
    start(ocopies)
    row0 = core * 128 + fb * 64 + sb * 32
    small = copies([(nw_hbm, nwb), (cw_hbm, cwb), (cb_hbm, cbb), (wx_hbm.at[1], wx), (cs_hbm.at[1], cs),
                    (resid.at[rows(row0, 32)], rmine)], lsem)
    start(small)
    stream = WeightStream(1, w_in, raw, w, wsem)
    pieces = iter(range(NW))
    lay_out = lambda: stream.lay_out(next(pieces))
    reduce_scatter(where, await_peers, yg, wout, ocopies, own, tx0, rx0, tx1, rx1, tx2, rx2, rsem, stream.begin, lay_out)
    wait(small)
    nw[...] = nwb[1:2, :].astype(F32)
    for sub, whole, part in my_rows(where):
        o = own[sub, :]
        oshard[part, :] = o
        v = o + rmine[part, :]
        scale = lax.rsqrt(jnp.mean(v * v, axis=-1, keepdims=True) + 1e-5)
        h[whole, :] = (v * scale * nw[...]).astype(BF16)
    for i in pieces:
        stream.lay_out(i)
    scopies = state_copies(1, st_hbm, st, ssem)
    start(scopies)
    acc[...] = jnp.zeros_like(acc)
    per = CW // KD
    all_gather(where, h, gsem, lambda c: proj_steps(c * per, (c + 1) * per, 0, acc, h, w))
    in_tail(1, where, acc, h, w, cs, (cwb, cbb, cw, cb), wx, x, xc, z, p, ptx, prx, psem)
    wait(scopies)


def last_kernel(yg, oshard, w_out, resid, out, wout, own, tx0, rx0, tx1, rx1, tx2, rx2, total, rbuf, osem, lsem, rsem, gsem):
    where = place()
    core, fb, sb, partner, first, second = where
    await_peers = enter((partner, first, second))
    ocopies = w_out_copies(1, w_out, wout, osem)
    start(ocopies)
    rcopy = pltpu.make_async_copy(resid, rbuf, lsem.at[0])
    reduce_scatter(where, await_peers, yg, wout, ocopies, own, tx0, rx0, tx1, rx1, tx2, rx2, rsem, rcopy.start, lambda: None)
    for sub, whole, part in my_rows(where):
        total[whole, :] = (own[sub, :] + oshard[part, :]).astype(BF16)
    rcopy.wait()

    def consume(c):
        col = pl.ds(c * CW, CW)

        def block(i, carry):
            r = rows(i * 32, 32)
            out[r, col] = rbuf[r, col] + total[r, col].astype(F32)
            return carry

        lax.fori_loop(0, TOK // 32, block, 0)

    all_gather(where, total, gsem, consume)


def ssm_kernel(layer, x, xc, z, p, cs, st, wdt_hbm, bdt_hbm, alog_hbm, dskip_hbm, st_hbm, *refs):
    if layer:
        refs = refs[2:]
    yg, conv_out, st_out, new, dts, us, ys, a, bc, wdt, bdt, dskip, bdt1, dskip1, lsem, osem, csem, isem = refs
    small = copies([(bdt_hbm, bdt), (dskip_hbm, dskip), (alog_hbm.at[layer], a), (wdt_hbm.at[layer], wdt)], lsem)
    start(small)
    ahead = AHEAD[layer]
    start(state_copies(layer, st_hbm, new, isem, ahead, NB))
    couts = copies([(cs.at[pl.ds(1, 2)], conv_out.at[layer, pl.ds(0, 2)]), (x, conv_out.at[layer, 2])], csem)
    start(couts)
    for hf in range(2):
        for k in range(2):
            v = p[hf, RANK + k * NST:RANK + (k + 1) * NST, :]
            bc[hf, k * NST:(k + 1) * NST, :] = v * lax.rsqrt(jnp.mean(v * v, axis=0, keepdims=True) + 1e-6)
    wait(small)
    a[...] = -jnp.exp(a[...])
    bdt1[...] = bdt[layer:layer + 1, :]
    dskip1[...] = dskip[layer:layer + 1, :]
    for hf in range(2):
        low = p[hf, 0:RANK, :]
        low = low * lax.rsqrt(jnp.mean(low * low, axis=0, keepdims=True) + 1e-6)
        dts[hf * (NB // 2):(hf + 1) * (NB // 2)] = lax.dot_general(
            low.astype(BF16), wdt[...], (((0,), (0,)), ((), ())), preferred_element_type=F32).reshape(NB // 2, TB, CH)

    def dt_block(i, carry):
        dt = jax.nn.softplus(dts[i] + bdt1[...])
        dts[i] = dt
        us[i] = dt * xc[rows(i * TB, TB), :].astype(F32)
        return carry

    lax.fori_loop(0, NB, dt_block, 0)
    row = lax.broadcasted_iota(jnp.int32, (8, CH), 0)

    def merge(level, one, two):
        k = 1 << level
        even = (row & k) == 0
        return jnp.where(even, one, two) + pltpu.roll(jnp.where(even, two, one), 8 - k, 0)

    def out_copy(i):
        r = rows(i * TB, TB)
        return pltpu.make_async_copy(new.at[r], st_out.at[layer, r], osem.at[i])

    def block(src, i, carry):
        r = rows(i * TB, TB)
        if src is new:
            pltpu.make_async_copy(st_hbm.at[layer, r], new.at[r], isem.at[i - ahead]).wait()
        hf = lax.div(i, NB // 2)
        shift = lax.rem(128 - lax.rem(i, NB // 2) * TB, 128)
        bct = pltpu.roll(bc[hf], shift, 1)
        for g in range(TB // 8):
            stack = []
            for j in range(g * 8, g * 8 + 8):
                bx = bct[0:NST, j:j + 1]
                cx = bct[NST:2 * NST, j:j + 1]
                s = jnp.exp(dts[i, j:j + 1, :] * a[...]) * src[i * TB + j] + us[i, j:j + 1, :] * bx
                new[i * TB + j] = s
                sc = s * cx
                level, v = 0, sc[0:8, :] + sc[8:16, :]
                while stack and stack[-1][0] == level:
                    v = merge(level, stack.pop()[1], v)
                    level += 1
                stack.append((level, v))
            ys[g * 8:g * 8 + 8, :] = stack[0][1]
        out_copy(i).start()
        zf = z[r, :].astype(F32)
        y = ys[...] + dskip1[...] * xc[r, :].astype(F32)
        yg[r, :] = (y * (zf * jax.nn.sigmoid(zf))).astype(BF16)
        return carry

    lax.fori_loop(0, ahead, functools.partial(block, st), 0)
    if ahead < NB:
        lax.fori_loop(ahead, NB, functools.partial(block, new), 0)
    wait(couts)
    for i in range(NB):
        out_copy(i).wait()


def sds(shape, dtype):
    return jax.ShapeDtypeStruct(shape, dtype)


def in_outs(layer):
    return (pltpu.VMEM((TOK, CH), BF16),) * 3 + (
        pltpu.VMEM((2, PW, 128), F32), pltpu.VMEM((3, TOK, CH), BF16), pltpu.VMEM((AHEAD[layer] * TB, NST, CH), F32))


def proj_scratch(slots):
    return [pltpu.VMEM((TOK, DIM), BF16), pltpu.VMEM((slots, DIM // NW, 2, CH), BF16), pltpu.VMEM((2 * DIM, CH), BF16),
            pltpu.VMEM((TOK, CH), F32)]


P_SCRATCH = [pltpu.VMEM((PW, CH), BF16), pltpu.VMEM((2, DIM), BF16), pltpu.VMEM((1, DIM), F32),
             pltpu.VMEM((2, 4, CH), BF16), pltpu.VMEM((2, CH), BF16), pltpu.VMEM((4, CH), F32), pltpu.VMEM((1, CH), F32),
             pltpu.VMEM((4, PW, 128), BF16), pltpu.VMEM((4, PW, 128), BF16)]
RS_SCRATCH = [pltpu.VMEM((CH, DIM), BF16), pltpu.VMEM((128, DIM), F32)] + [pltpu.VMEM((n, DIM), BF16) for n in (128, 128, 64, 64, 32, 32)]


def params(mib, collective_id=None):
    if collective_id is None:
        return pltpu.CompilerParams(vmem_limit_bytes=int(mib * 2 ** 20))
    return pltpu.CompilerParams(vmem_limit_bytes=int(mib * 2 ** 20), collective_id=collective_id, has_side_effects=True)


def solution(mesh):
    def first_call(residual, *args):
        return pl.pallas_call(
            first_kernel, out_shape=in_outs(0), in_specs=[ANY] * 8, out_specs=(VMEM,) * 6,
            scratch_shapes=[*proj_scratch(4), pltpu.VMEM((TOK, DIM), F32), *P_SCRATCH,
                            DMA((NW,)), DMA((8,)), DMA((5,)), DMA((NB,)), DMA((2, 4))],
            compiler_params=params(41.25, 0), name="first",
        )(residual, *args)

    def middle_call(yg, w_out, residual, *args):
        return pl.pallas_call(
            middle_kernel, out_shape=(*in_outs(1), pltpu.VMEM((32, DIM), F32)),
            in_specs=[VMEM] + [ANY] * 9, out_specs=(VMEM,) * 7,
            scratch_shapes=[*RS_SCRATCH, pltpu.VMEM((32, DIM), F32), *proj_scratch(2), *P_SCRATCH,
                            DMA((NCH,)), DMA((NW,)), DMA((6,)), DMA((NB,)), DMA((2, 3 * NCH)), DMA((2, 3 * NCH)), DMA((2, 4))],
            compiler_params=params(46, 1), name="middle",
        )(yg, w_out, residual, *args)

    def last_call(yg, oshard, w_out, residual):
        return pl.pallas_call(
            last_kernel, out_shape=pltpu.VMEM((TOK, DIM), F32), in_specs=[VMEM, VMEM, ANY, ANY], out_specs=VMEM,
            scratch_shapes=[*RS_SCRATCH, pltpu.VMEM((TOK, DIM), BF16), pltpu.VMEM((TOK, DIM), F32),
                            DMA((NCH,)), DMA((1,)), DMA((2, 3 * NCH)), DMA((2, 3 * NCH))],
            compiler_params=params(52, 2), name="last",
        )(yg, oshard, w_out, residual)

    def ssm_call(layer, held, shapes, *args):
        return pl.pallas_call(
            functools.partial(ssm_kernel, layer),
            out_shape=(pltpu.VMEM((TOK, CH), BF16), *shapes),
            in_specs=[VMEM] * 6 + [ANY] * (5 + len(held)), out_specs=(VMEM, ANY, ANY),
            input_output_aliases={11: 1, 12: 2} if held else {},
            scratch_shapes=[pltpu.VMEM((TOK, NST, CH), F32), pltpu.VMEM((NB, TB, CH), F32),
                            pltpu.VMEM((NB, TB, CH), F32), pltpu.VMEM((TB, CH), F32), pltpu.VMEM((NST, CH), F32),
                            pltpu.VMEM((2, 2 * NST, 128), F32), pltpu.VMEM((RANK, CH), BF16),
                            pltpu.VMEM((2, CH), F32), pltpu.VMEM((2, CH), F32), pltpu.VMEM((1, CH), F32), pltpu.VMEM((1, CH), F32),
                            DMA((4,)), DMA((NB,)), DMA((2,)), DMA((NB,))],
            compiler_params=params(22), name=f"ssm{layer}",
        )(*args, *held)

    def device_step(residual, norm_w, w_in, conv_w, conv_b, w_x, w_dt, b_dt, a_log, d_skip, w_out, conv_state, ssm_state):
        cs = jnp.swapaxes(conv_state, 1, 2)
        wx = jnp.swapaxes(w_x, 1, 2)
        shapes = (sds(cs.shape, BF16), sds(ssm_state.shape, F32))
        in_args = (residual, norm_w, w_in, conv_w, conv_b, wx, cs, ssm_state)
        ssm_args = (w_dt, b_dt, a_log, d_skip, ssm_state)
        yg, *held = ssm_call(0, (), shapes, *first_call(*in_args), *ssm_args)
        *mid, oshard = middle_call(yg, w_out, *in_args)
        yg, conv_out, ssm_out = ssm_call(1, tuple(held), shapes, *mid, *ssm_args)
        return last_call(yg, oshard, w_out, residual), jnp.swapaxes(conv_out, 1, 2), ssm_out

    cache_spec = P(None, 'dp', None, 'tp')
    in_specs = (P('dp', None), P(None, None), P(None, None, None, 'tp'), P(None, None, 'tp'), P(None, 'tp'), P(None, 'tp', None), P(None, None, 'tp'), P(None, 'tp'), P(None, None, 'tp'), P(None, 'tp'), P(None, 'tp', None), cache_spec, cache_spec)
    out_specs = (P('dp', None), cache_spec, cache_spec)
    return jax.shard_map(device_step, mesh=mesh, in_specs=in_specs, out_specs=out_specs, check_vma=False)
```
